32 devices in a mesh: depth: 16 (over z, y, core), chan: 2 (over x).
Axes of the slice: x: 2, y: 2, z: 4, core: 2. Of those that a mesh axis runs over, the one named last changes fastest.
Arguments:
- pre: float32 [1, 512, 32, 256], P(None, 'chan', 'depth'), may hold values from -6 to 6
- grad_out: float32 [1, 512, 32, 256], P(None, 'chan', 'depth'), may hold values from -6 to 6
- weight: float32 [27, 512, 512], P(None, 'chan'), may hold values from -0.0546875 to 0.0546875
Outputs:
- grad_pre: float32 [1, 512, 32, 256], P(None, 'chan', 'depth')
- grad_weight: float32 [27, 512, 512], P(None, 'chan', 'depth')
The draws below stay inside these ranges and needn't reach their ends.
All inputs are finite; a program needn't handle non-finite values.
Results may differ from the reference program's by a relative error of at most 0.0001.
Values sent between devices are 32-bit elements; how exact they have to be, the bound alone decides.
A program may use at most 192 MiB of HBM per device.

```python
import math
import jax
import jax.numpy as jnp
from jax import lax

C = 512
W = 16
BATCH = 1
PLANE = 256
DEPTH = 32
VOXELS = 8192


def strengthened(result, stream_key, source, target, blocks, factor):
    owner, partner = [(jnp.arange(result.shape[position]) // (result.shape[position] // blocks)).reshape([-1 if axis == position else 1 for axis in range(result.ndim)]) for position in (source, target)]
    chosen = jax.random.permutation(stream_key, blocks)[partner]
    strong = (owner == chosen) | (owner == (partner + blocks // 2) % blocks)
    return jnp.where(strong, factor * result, result)


def shard_levels(stream_key, dims, shards, low, top_value):
    level, own = 1.0, jax.random.fold_in(stream_key, 6)
    for dim, blocks in shards:
        draws = jnp.exp(jax.random.uniform(jax.random.fold_in(own, dim), (blocks,), jnp.float32, low / len(shards), top_value / len(shards)))
        level = level * jnp.repeat(draws, dims[dim] // blocks).reshape([-1 if axis == dim else 1 for axis in range(len(dims))])
    return level


def normal_values(stream_key, extent, width, reach, split=(), kind=jnp.bfloat16):
    drawn = width * jax.random.normal(stream_key, extent, jnp.float32)
    if split:
        drawn = drawn * shard_levels(stream_key, extent, split, -0.22, 0.18)
    return jnp.clip(drawn, -reach, reach).astype(kind)


def gaussian_with(own_key, extent, deviation, reach, pieces, heavy, dtype=jnp.bfloat16):
    entries = deviation * jax.random.normal(own_key, extent, jnp.float32)
    if pieces:
        entries = entries * shard_levels(own_key, extent, pieces, -0.22, 0.18)
    return jnp.clip(strengthened(entries, jax.random.fold_in(own_key, 3), *heavy), -reach, reach).astype(dtype)


def setup_inputs(seed: int = 0) -> dict:
    arg_keys = jax.random.split(jax.random.key(seed), 4)
    pre = normal_values(arg_keys[0], (BATCH, C, DEPTH, PLANE), 1.0, 6.0, ((1, 2), (2, 16)), jnp.float32)
    grad_out = gaussian_with(arg_keys[1], (BATCH, C, DEPTH, PLANE), 1.0, 6.0, ((1, 2), (2, 16)), (2, 1, 16, 2.0), jnp.float32)
    weight = normal_values(arg_keys[2], (27, C, C), (27 * C) ** -0.5, 0.0546875, ((1, 2),), jnp.float32)
    return {"pre": pre, "grad_out": grad_out, "weight": weight}


def shift_plane(block, drow, dcol):
    plane = block.shape[-1]
    step = drow * W + dcol
    lead = [(0, 0)] * (block.ndim - 1)
    if step > 0:
        moved = jnp.pad(block[..., step:], lead + [(0, step)])
    elif step < 0:
        moved = jnp.pad(block[..., :plane + step], lead + [(-step, 0)])
    else:
        moved = block
    column = jnp.arange(plane) % W
    valid = (column + dcol >= 0) & (column + dcol < W)
    return jnp.where(valid, moved, jnp.float32(0.0))

def normal_cdf(value):
    return 0.5 * (1.0 + jax.scipy.special.erf(value / math.sqrt(2.0)))

def reference(pre, grad_out, weight):
    act = pre * normal_cdf(pre)
    depth_pad = [(0, 0), (0, 0), (1, 1), (0, 0)]
    act_pad = jnp.pad(act, depth_pad)
    cot_pad = jnp.pad(grad_out, depth_pad)
    grad_act = jnp.zeros(pre.shape, jnp.float32)
    filters = []
    for depth_off in range(3):
        for row_off in range(3):
            for col_off in range(3):
                index = 9 * depth_off + 3 * row_off + col_off
                source = shift_plane(act_pad[:, :, depth_off:depth_off + DEPTH], row_off - 1, col_off - 1)
                filters.append(jnp.einsum('bcdp,bodp->co', source, grad_out, precision=lax.Precision.HIGHEST))
                moved = shift_plane(cot_pad[:, :, 2 - depth_off:2 - depth_off + DEPTH], 1 - row_off, 1 - col_off)
                grad_act = grad_act + jnp.einsum('co,bodp->bcdp', weight[index], moved, precision=lax.Precision.HIGHEST)
    slope = normal_cdf(pre) + pre * jnp.exp(-0.5 * pre * pre) / math.sqrt(2.0 * math.pi)
    grad_pre = grad_act * slope
    grad_weight = jnp.stack(filters) * float(VOXELS) ** (-0.5)
    return (grad_pre, grad_weight)
```

```python
import math

import jax
import jax.numpy as jnp
from jax import lax
from jax.sharding import PartitionSpec as P

W = 16


def with_halo(x, sides, width):
    for axis, dim in sides:
        size, length = (lax.axis_size(axis), x.shape[dim])
        up = [(i, (i + 1) % size) for i in range(size - 1)]
        down = [(j, i) for i, j in up]
        last = lax.slice_in_dim(x, length - width, length, axis=dim)
        first = lax.slice_in_dim(x, 0, width, axis=dim)
        before = lax.ppermute(last, axis, up)
        after = lax.ppermute(first, axis, down)
        x = jnp.concatenate([before, x, after], axis=dim)
    return x


def shift_plane(block, drow, dcol):
    plane = block.shape[-1]
    step = drow * W + dcol
    lead = [(0, 0)] * (block.ndim - 1)
    if step > 0:
        moved = jnp.pad(block[..., step:], lead + [(0, step)])
    elif step < 0:
        moved = jnp.pad(block[..., : plane + step], lead + [(-step, 0)])
    else:
        moved = block
    column = jnp.arange(plane) % W
    valid = (column + dcol >= 0) & (column + dcol < W)
    return jnp.where(valid, moved, jnp.float32(0.0))


def normal_cdf(value):
    return 0.5 * (1.0 + jax.scipy.special.erf(value / math.sqrt(2.0)))


def transposed(weight, padded_piece, out_planes):
    total = jnp.zeros(
        (padded_piece.shape[0], weight.shape[1], out_planes, padded_piece.shape[3]), jnp.float32
    )
    for depth_off in range(3):
        layer = padded_piece[:, :, 2 - depth_off : 2 - depth_off + out_planes]
        for row_off in range(3):
            moved = jnp.stack(
                [shift_plane(layer, 1 - row_off, 1 - col_off) for col_off in range(3)]
            )
            first = 9 * depth_off + 3 * row_off
            total = total + jnp.einsum(
                "kco,kbodp->bcdp", weight[first : first + 3], moved, precision=lax.Precision.HIGH
            )
    return total


def group_size(count):
    return math.gcd(count, 4)


def shards(pre, grad_out, weight):
    batch, width_blk, planes, plane = pre.shape
    count = lax.axis_size("depth")
    near = group_size(count)
    far = count // near
    blocks = [[f * near + n for n in range(near)] for f in range(far)]
    strides = [[f * near + n for f in range(far)] for n in range(near)]
    near_pre = lax.all_gather(pre, "depth", axis=2, tiled=True, axis_index_groups=blocks)
    whole = lax.all_gather(grad_out, "chan", axis=1, tiled=True)
    outs = whole.shape[1]
    part = outs // count
    split = whole.reshape(batch, far, near, part, planes, plane)
    mine = lax.all_to_all(split, "depth", 2, 3, axis_index_groups=blocks)
    mine = mine.reshape(batch, far * part, near * planes, plane)
    up = [(i, i + near) for i in range(count - near)]
    down = [(j, i) for i, j in up]
    last = lax.ppermute(mine[:, :, -1:], "depth", up)
    first = lax.ppermute(mine[:, :, :1], "depth", down)
    rim = jnp.concatenate([last, mine, first], axis=2)
    span = near * planes
    act = near_pre * normal_cdf(near_pre)
    moved = jnp.stack(
        [shift_plane(rim, 1 - kh, 1 - kw) for kh in range(3) for kw in range(3)]
    )
    filt = jnp.concatenate(
        [
            jnp.einsum(
                "bcdp,kbodp->kco", act, moved[:, :, :, 2 - kd : 2 - kd + span], precision=lax.Precision.HIGH
            )
            for kd in range(3)
        ]
    )
    summed = lax.psum_scatter(
        filt, "depth", scatter_dimension=2, tiled=True, axis_index_groups=strides
    )
    rimmed = with_halo(whole, (("depth", 2),), 1)
    grad_act = transposed(weight, rimmed, planes)
    slope = normal_cdf(pre) + pre * jnp.exp(-0.5 * pre * pre) / math.sqrt(2.0 * math.pi)
    grad_pre = grad_act * slope
    voxel_count = batch * planes * count * plane
    grad_weight = summed * float(voxel_count) ** (-0.5)
    return (grad_pre, grad_weight)


def solution(mesh):
    placed = (P(None, "chan", "depth", None), P(None, "chan", "depth", None), P(None, "chan", None))
    return jax.shard_map(
        shards,
        mesh=mesh,
        in_specs=placed,
        out_specs=(P(None, "chan", "depth", None), P(None, "chan", "depth")),
        check_vma=False,
    )
```
